32 devices in a mesh: dp: 2 (over x), tp: 4 (over z), cp: 4 (over y, core).
Axes of the slice: x: 2, y: 2, z: 4, core: 2. Of those that a mesh axis runs over, the one named last changes fastest.
Arguments:
- hidden: bfloat16 [8192, 5120], P(('dp', 'cp')), parts along dimension 0
- norm_scale: float32 [5120], replicated
- w_qkv: bfloat16 [5120, 6144], P(None, 'tp')
- w_out: bfloat16 [4096, 5120], P('tp')
Outputs:
- output 1: bfloat16 [8192, 5120], P(('dp', 'cp')), parts along dimension 0
- output 2: bfloat16 [8192, 8, 128], P(('dp', 'cp'), 'tp'), parts along dimension 0
- output 3: bfloat16 [8192, 8, 128], P(('dp', 'cp'), 'tp'), parts along dimension 0
There are 2 independent parts. The reference program is written for one: setup_inputs(seed, part) draws one part's arguments, and reference() takes and returns one part's arrays. A program takes and returns all parts, laid end to end along the dimension named above; an argument that names none is the same for every part.
All inputs are finite; a program needn't handle non-finite values.
Results may differ from the reference program's by a relative error of at most 0.00914097.
Values are sent between devices in bfloat16 or wider.
A program may use at most 1 GiB of HBM per device.

```python
import math
import jax
import jax.numpy as jnp
from jax import lax

MODEL_DIM = 5120
Q_HEADS = 32
KV_HEADS = 8
HEAD_DIM = 128
SEQ_LEN = 4096

GROUP_SIZE = Q_HEADS // KV_HEADS
QKV_COLS = (Q_HEADS + 2 * KV_HEADS) * HEAD_DIM
ATTN_COLS = Q_HEADS * HEAD_DIM
Q_BLOCK = math.gcd(SEQ_LEN, 128)
N_BLOCKS = SEQ_LEN // Q_BLOCK
ROPE_BASE = 500000.0
NORM_EPS = 1e-5
CLIP_VALUE = 8.0
Q_GAIN = 3.5
K_GAIN = 0.35
V_GAIN = 3.5
OUT_GAIN = math.sqrt(SEQ_LEN / (10.0 * math.log(SEQ_LEN))) / 4.0


def column_gains():
    one_group = jnp.concatenate([
        jnp.full((GROUP_SIZE * HEAD_DIM,), Q_GAIN, jnp.float32),
        jnp.full((HEAD_DIM,), K_GAIN, jnp.float32),
        jnp.full((HEAD_DIM,), V_GAIN, jnp.float32),
    ])
    return jnp.tile(one_group, KV_HEADS)


def setup_inputs(seed: int = 0, part: int = 0) -> dict:
    part_key = jax.random.fold_in(jax.random.key(seed), part)
    key_norm, key_qkv, key_out = jax.random.split(jax.random.key(seed + 1), 3)
    hidden = jax.random.normal(part_key, (SEQ_LEN, MODEL_DIM), jnp.float32).astype(jnp.bfloat16)
    norm_scale = 1.0 + 0.5 * jax.random.normal(key_norm, (MODEL_DIM,), jnp.float32)
    w_qkv = (jax.random.normal(key_qkv, (MODEL_DIM, QKV_COLS), jnp.float32) * (column_gains() * MODEL_DIM ** -0.5)).astype(jnp.bfloat16)
    w_out = (jax.random.normal(key_out, (ATTN_COLS, MODEL_DIM), jnp.float32) * (OUT_GAIN * ATTN_COLS ** -0.5)).astype(jnp.bfloat16)
    return {"hidden": hidden, "norm_scale": norm_scale, "w_qkv": w_qkv, "w_out": w_out}


def layer_norm(hidden, norm_scale):
    hidden_f32 = hidden.astype(jnp.float32)
    centred = hidden_f32 - jnp.mean(hidden_f32, axis=-1, keepdims=True)
    variance = jnp.mean(centred * centred, axis=-1, keepdims=True)
    return (centred * lax.rsqrt(variance + NORM_EPS) * norm_scale).astype(jnp.bfloat16)


def rope_tables(positions):
    inv_freq = 1.0 / (ROPE_BASE ** (jnp.arange(0, HEAD_DIM, 2, dtype=jnp.float32) / HEAD_DIM))
    angles = positions.astype(jnp.float32)[:, None] * inv_freq[None, :]
    return jnp.cos(angles), jnp.sin(angles)


def rotate(tensor, cos_table, sin_table):
    tensor_f32 = tensor.astype(jnp.float32)
    half_dim = tensor_f32.shape[-1] // 2
    first_half = tensor_f32[..., :half_dim]
    second_half = tensor_f32[..., half_dim:]
    return jnp.concatenate([first_half * cos_table - second_half * sin_table, second_half * cos_table + first_half * sin_table], axis=-1).astype(jnp.bfloat16)


def reference(hidden, norm_scale, w_qkv, w_out):
    normed = layer_norm(hidden, norm_scale)
    qkv_all = jnp.clip(jnp.dot(normed, w_qkv, preferred_element_type=jnp.float32).astype(jnp.bfloat16), -CLIP_VALUE, CLIP_VALUE)
    qkv_all = qkv_all.reshape(SEQ_LEN, KV_HEADS, GROUP_SIZE + 2, HEAD_DIM)
    cos_table, sin_table = rope_tables(jnp.arange(SEQ_LEN))
    queries = rotate(qkv_all[:, :, :GROUP_SIZE, :], cos_table[:, None, None, :], sin_table[:, None, None, :])
    key_cache = rotate(qkv_all[:, :, GROUP_SIZE, :], cos_table[:, None, :], sin_table[:, None, :])
    value_cache = qkv_all[:, :, GROUP_SIZE + 1, :]
    q_items = queries.reshape(N_BLOCKS, Q_BLOCK, KV_HEADS, GROUP_SIZE, HEAD_DIM).transpose(2, 0, 1, 3, 4).reshape(KV_HEADS * N_BLOCKS, Q_BLOCK, GROUP_SIZE, HEAD_DIM)
    head_ids = jnp.repeat(jnp.arange(KV_HEADS), N_BLOCKS)
    block_ids = jnp.tile(jnp.arange(N_BLOCKS), KV_HEADS)
    key_heads = key_cache.transpose(1, 0, 2)
    value_heads = value_cache.transpose(1, 0, 2)
    key_pos = jnp.arange(SEQ_LEN)

    def one_item(item_args):
        q_blk, head_id, block_id = item_args
        key_blk = key_heads[head_id].astype(jnp.float32)
        val_blk = value_heads[head_id].astype(jnp.float32)
        scores = jnp.einsum("qrd,kd->rqk", q_blk.astype(jnp.float32), key_blk) * (HEAD_DIM ** -0.5)
        q_pos = block_id * Q_BLOCK + jnp.arange(Q_BLOCK)
        scores = jnp.where(key_pos[None, None, :] <= q_pos[None, :, None], scores, -jnp.inf)
        weights = jax.nn.softmax(scores, axis=-1)
        return jnp.einsum("rqk,kd->qrd", weights, val_blk).astype(jnp.bfloat16)

    attn_out = lax.map(one_item, (q_items, head_ids, block_ids))
    attn_out = attn_out.reshape(KV_HEADS, N_BLOCKS, Q_BLOCK, GROUP_SIZE, HEAD_DIM).transpose(1, 2, 0, 3, 4).reshape(SEQ_LEN, ATTN_COLS)
    out_proj = jnp.dot(attn_out, w_out, preferred_element_type=jnp.float32)
    h_out = (hidden.astype(jnp.float32) + out_proj).astype(jnp.bfloat16)
    return (h_out, key_cache, value_cache)
```

```python
import functools

import jax
import jax.numpy as jnp
from jax import lax
from jax.experimental import pallas as pl
from jax.experimental.pallas import tpu as pltpu
from jax.sharding import PartitionSpec as P

HEAD_DIM = 128
ROPE_BASE = 500000.0
NORM_EPS = 1e-5
CLIP_VALUE = 8.0
MASK_VALUE = -1e30
SCALE2 = HEAD_DIM ** -0.5 * 1.4426950408889634

ROWS = 1024
CHUNK = 256
N_CHUNKS = ROWS // CHUNK
DIM = 5120
GROUP_COLS = 768


def rope_tables(positions):
    inv_freq = 1.0 / (ROPE_BASE ** (jnp.arange(0, HEAD_DIM, 2, dtype=jnp.float32) / HEAD_DIM))
    angles = positions.astype(jnp.float32)[:, None] * inv_freq[None, :]
    cos, sin = jnp.cos(angles), jnp.sin(angles)
    return jnp.concatenate([cos, cos], axis=-1), jnp.concatenate([-sin, sin], axis=-1)


def rope(x, cos, sin):
    return (x * cos + pltpu.roll(x, HEAD_DIM // 2, 1) * sin).astype(jnp.bfloat16)


def clipped(acc):
    return jnp.clip(acc.astype(jnp.bfloat16), -CLIP_VALUE, CLIP_VALUE)


def kv_kernel(h_ref, scale_ref, w0_ref, w1_ref, cos_ref, sin_ref, normed_ref, kv_ref):
    x = h_ref[...].astype(jnp.float32)
    centred = x - jnp.mean(x, axis=-1, keepdims=True)
    variance = jnp.mean(centred * centred, axis=-1, keepdims=True)
    normed = (centred * lax.rsqrt(variance + NORM_EPS) * scale_ref[...]).astype(jnp.bfloat16)
    normed_ref[...] = normed
    for g, w_ref in enumerate((w0_ref, w1_ref)):
        y = clipped(jnp.dot(normed, w_ref[...], preferred_element_type=jnp.float32))
        kv_ref[:, g * 256:g * 256 + 128] = rope(y[:, :128].astype(jnp.float32), cos_ref[...], sin_ref[...])
        kv_ref[:, g * 256 + 128:g * 256 + 256] = y[:, 128:]


def q_kernel(n_ref, w0_ref, w1_ref, w2_ref, w3_ref, cos_ref, sin_ref, q_ref):
    for i, w_ref in enumerate((w0_ref, w1_ref, w2_ref, w3_ref)):
        y = clipped(jnp.dot(n_ref[...], w_ref[...], preferred_element_type=jnp.float32)).astype(jnp.float32)
        for h in range(2):
            q_ref[:, i * 256 + h * 128:i * 256 + h * 128 + 128] = rope(y[:, h * 128:h * 128 + 128], cos_ref[...], sin_ref[...])


def attn_kernel(chunk, cp_ref, q_ref, kv_ref, a1_ref, b0_ref, b1_ref, o_ref, acc_ref, m_ref, l_ref):
    cp = cp_ref[0]
    q = jnp.concatenate([q_ref[:, h * 128:h * 128 + 128] for h in range(4)], axis=0)
    acc_ref[...] = jnp.zeros_like(acc_ref)
    m_ref[...] = jnp.full_like(m_ref, MASK_VALUE)
    l_ref[...] = jnp.zeros_like(l_ref)

    def tile(ref, start, width, masked):
        k = ref[pl.ds(start, width), :128]
        v = ref[pl.ds(start, width), 128:]
        s = lax.dot_general(q, k, (((1,), (1,)), ((), ())), preferred_element_type=jnp.float32) * SCALE2
        if masked:
            row = lax.broadcasted_iota(jnp.int32, s.shape, 0) % CHUNK
            col = lax.broadcasted_iota(jnp.int32, s.shape, 1)
            s = jnp.where(col <= row, s, MASK_VALUE)
        m_old = m_ref[...]
        m_new = jnp.maximum(m_old, jnp.max(s, axis=-1, keepdims=True))
        rescale = jnp.exp2(m_old - m_new)
        p = jnp.exp2(s - jnp.concatenate([m_new] * (width // 128), axis=1))
        m_ref[...] = m_new
        part = p[:, :128]
        for j in range(1, width // 128):
            part = part + p[:, j * 128:j * 128 + 128]
        l_ref[...] = l_ref[...] * rescale + part
        acc_ref[...] = acc_ref[...] * rescale + jnp.dot(p.astype(jnp.bfloat16), v, preferred_element_type=jnp.float32)

    tile(kv_ref, chunk * CHUNK, CHUNK, True)
    if chunk % 2:
        tile(kv_ref, (chunk - 1) * CHUNK, CHUNK, False)
    for j in range(chunk // 2):
        tile(kv_ref, j * 512, 512, False)

    def whole(ref, on):
        def body(t, _):
            tile(ref, pl.multiple_of(t * 512, 512), 512, False)
            return 0
        lax.fori_loop(0, jnp.where(on, ROWS // 512, 0), body, 0)

    whole(a1_ref, cp % 2 == 1)
    whole(b0_ref, cp >= 2)
    whole(b1_ref, cp >= 2)
    out = (acc_ref[...] / jnp.sum(l_ref[...], axis=-1, keepdims=True)).astype(jnp.bfloat16)
    for h in range(4):
        o_ref[:, h * 128:h * 128 + 128] = out[h * CHUNK:(h + 1) * CHUNK]


N_TILE = 512
PIECES = 11


def proj_kernel(aliased, p_ref, *refs):
    o_refs, hid_ref, w_own = refs[:4], refs[4], refs[5]
    pieces = refs[6:6 + 30]
    out_ref, wbuf, sems = refs[-3:]
    j = pl.program_id(0)
    p = p_ref[0]

    def start(tile, slot):
        cols = pl.ds(pl.multiple_of(tile * N_TILE, N_TILE), N_TILE)

        def put(src, row, n):
            pltpu.make_async_copy(src.at[:, cols], wbuf.at[slot, pl.ds(row, n), :], sems.at[slot]).start()

        put(w_own, 0, ROWS)
        for k in range(3):
            for core in range(2):
                whole = pieces[k * 10 + core * 5:k * 10 + core * 5 + 5]
                for flip, src in zip((0, 4, 2), whole[:3]):
                    put(src, pl.multiple_of((k + 1) * ROWS + (p ^ (flip + core)) * 128, 128), 128)
                diag = pl.multiple_of((k + 1) * ROWS + (p ^ (6 + core)) * 128, 128)
                put(whole[3], diag, 64)
                put(whole[4], pl.multiple_of(diag + 64, 64), 64)

    @pl.when(j == 0)
    def _():
        start(0, 0)

    slot = lax.rem(j, 2)

    @pl.when(j + 1 < pl.num_programs(0))
    def _():
        start(j + 1, 1 - slot)

    pltpu.make_async_copy(wbuf.at[slot], wbuf.at[slot], sems.at[slot]).wait()
    acc = jnp.dot(o_refs[0][...], wbuf[slot, 0:ROWS, :], preferred_element_type=jnp.float32)
    for k in range(1, 4):
        acc = acc + jnp.dot(o_refs[k][...], wbuf[slot, k * ROWS:(k + 1) * ROWS, :], preferred_element_type=jnp.float32)
    out_ref[...] = (hid_ref[...].astype(jnp.float32) + acc).astype(jnp.bfloat16)


def cost(flops, nbytes):
    return pl.CostEstimate(flops=flops, bytes_accessed=nbytes, transcendentals=0)


def once(shape, index_map):
    return pl.BlockSpec(shape, index_map, pipeline_mode=pl.Buffered(1))


def project_kv(hidden, norm_scale, w_qkv, cos, sin):
    tm = 128
    row = lambda i: (i, 0)
    return pl.pallas_call(
        kv_kernel,
        grid=(ROWS // tm,),
        in_specs=[pl.BlockSpec((tm, DIM), row), once((1, DIM), lambda i: (0, 0)), once((DIM, 256), lambda i: (0, 2)), once((DIM, 256), lambda i: (0, 5)), pl.BlockSpec((tm, 128), row), pl.BlockSpec((tm, 128), row)],
        out_specs=[pl.BlockSpec((tm, DIM), row), pl.BlockSpec((tm, 512), row)],
        out_shape=[jax.ShapeDtypeStruct((ROWS, DIM), jnp.bfloat16), jax.ShapeDtypeStruct((ROWS, 512), jnp.bfloat16)],
        compiler_params=pltpu.CompilerParams(vmem_limit_bytes=48 * 2 ** 20),
        cost_estimate=cost(2 * ROWS * DIM * 512, 26 * 2 ** 20),
        name="kv_proj",
    )(hidden, norm_scale.reshape(1, DIM), w_qkv, w_qkv, cos, sin)


def project_q(normed, w_qkv, cos, sin):
    tm = 256
    row = lambda i: (i, 0)
    return pl.pallas_call(
        q_kernel,
        grid=(ROWS // tm,),
        in_specs=[pl.BlockSpec((tm, DIM), row)] + [once((DIM, 256), functools.partial(lambda b, i: (0, b), b)) for b in (0, 1, 3, 4)] + [pl.BlockSpec((tm, 128), row)] * 2,
        out_specs=pl.BlockSpec((tm, 1024), row),
        out_shape=jax.ShapeDtypeStruct((ROWS, 1024), jnp.bfloat16),
        compiler_params=pltpu.CompilerParams(vmem_limit_bytes=48 * 2 ** 20),
        cost_estimate=cost(2 * ROWS * DIM * 1024, 22 * 2 ** 20),
        name="q_proj",
    )(normed, w_qkv, w_qkv, w_qkv, w_qkv, cos, sin)


def attend(chunk, cp, q, kv, a1, b0, b1):
    blk = pl.BlockSpec((ROWS, 256), lambda g, s: (0, g))
    return pl.pallas_call(
        functools.partial(attn_kernel, chunk),
        grid_spec=pltpu.PrefetchScalarGridSpec(
            num_scalar_prefetch=1,
            grid=(2,),
            in_specs=[pl.BlockSpec((CHUNK, 512), lambda g, s: (chunk, g))] + [blk] * 4,
            out_specs=pl.BlockSpec((CHUNK, 512), lambda g, s: (0, g)),
            scratch_shapes=[pltpu.VMEM((4 * CHUNK, 128), jnp.float32)] * 3,
        ),
        out_shape=jax.ShapeDtypeStruct((CHUNK, 1024), jnp.bfloat16),
        compiler_params=pltpu.CompilerParams(vmem_limit_bytes=48 * 2 ** 20),
        cost_estimate=cost(12 * 10 ** 9, 6 * 2 ** 20),
        name=f"attn_{chunk}",
    )(cp, q, kv, a1, b0, b1)


def project_out(chunk, p, os, hidden, w_own, pieces, prev):
    o_spec = once((CHUNK, 1024), lambda j, s: (0, 0))
    tile = pl.BlockSpec((CHUNK, N_TILE), lambda j, s: (chunk, j))
    hbm = pl.BlockSpec(memory_space=pl.ANY)
    args = [p, *os, hidden, w_own, *pieces]
    specs = [o_spec] * 4 + [tile, hbm] + [hbm] * len(pieces)
    alias = {}
    if prev is not None:
        args.append(prev)
        specs.append(hbm)
        alias = {len(args) - 1: 0}
    return pl.pallas_call(
        functools.partial(proj_kernel, prev is not None),
        grid_spec=pltpu.PrefetchScalarGridSpec(
            num_scalar_prefetch=1,
            grid=(DIM // N_TILE,),
            in_specs=specs,
            out_specs=tile,
            scratch_shapes=[pltpu.VMEM((2, 4 * ROWS, N_TILE), jnp.bfloat16), pltpu.SemaphoreType.DMA((2,))],
        ),
        out_shape=jax.ShapeDtypeStruct((ROWS, DIM), jnp.bfloat16),
        input_output_aliases=alias,
        compiler_params=pltpu.CompilerParams(vmem_limit_bytes=56 * 2 ** 20),
        cost_estimate=cost(2 * CHUNK * 4 * ROWS * DIM, 48 * 2 ** 20),
        name=f"proj_{chunk}",
    )(*args)


def solution(mesh):
    tok_spec = P(("dp", "cp"), None)
    cache_spec = P(("dp", "cp"), "tp", None)
    ring = [(i, (i + 1) % 4) for i in range(4)]
    swap_x = functools.partial(lax.ppermute, axis_name="dp", perm=[(0, 1), (1, 0)])
    swap_y = functools.partial(lax.ppermute, axis_name="cp", perm=[(0, 2), (2, 0), (1, 3), (3, 1)])
    swap_core = functools.partial(lax.ppermute, axis_name="cp", perm=[(0, 1), (1, 0), (2, 3), (3, 2)])
    shift_z = functools.partial(lax.ppermute, axis_name="tp", perm=ring)

    def local_fn(hidden, norm_scale, w_qkv, w_out):
        cp = lax.axis_index("cp")
        p = lax.axis_index("dp") * 4 + cp
        cos, sin = rope_tables(cp * ROWS + jnp.arange(ROWS))

        w_slice = lax.dynamic_slice(w_out, (p * 128, 0), (128, DIM))
        r1 = shift_z(w_slice)
        r2 = shift_z(r1)
        r3 = shift_z(r2)

        normed, kv = project_kv(hidden, norm_scale, w_qkv, cos, sin)
        a1 = lax.ppermute(kv, "cp", [(0, 1), (2, 3)])
        b0 = lax.ppermute(kv, "cp", [(0, 2), (1, 3)])
        b1 = lax.ppermute(b0, "cp", [(2, 3), (3, 2)])
        q = project_q(normed, w_qkv, cos, sin)

        pieces = []
        for r in (r1, r2, r3):
            x, y = swap_x(r), swap_y(r)
            d1, d2 = swap_y(x[:64]), swap_x(y[64:])
            mine = [r, x, y, d1, d2]
            pieces += mine + [swap_core(v) for v in mine]

        cp_arr, p_arr = cp.reshape(1).astype(jnp.int32), p.reshape(1).astype(jnp.int32)
        h_out = None
        for c in range(N_CHUNKS):
            o = attend(c, cp_arr, q, kv, a1, b0, b1)
            os = [o]
            for _ in range(3):
                os.append(shift_z(os[-1]))
            h_out = project_out(c, p_arr, os, hidden, w_out, pieces, h_out)

        kv4 = kv.reshape(ROWS, 2, 2, HEAD_DIM)
        return h_out, kv4[:, :, 0], kv4[:, :, 1]

    return jax.shard_map(local_fn, mesh=mesh, in_specs=(tok_spec, P(None), P(None, "tp"), P("tp", None)), out_specs=(tok_spec, cache_spec, cache_spec), check_vma=False)
```

```python
import functools

import jax
import jax.numpy as jnp
from jax import lax
from jax.experimental import pallas as pl
from jax.experimental.pallas import tpu as pltpu
from jax.sharding import PartitionSpec as P

HEAD_DIM = 128
ROPE_BASE = 500000.0
NORM_EPS = 1e-5
CLIP_VALUE = 8.0
MASK_VALUE = -1e30
SCALE2 = HEAD_DIM ** -0.5 * 1.4426950408889634

ROWS = 1024
CHUNK = 256
N_CHUNKS = ROWS // CHUNK
DIM = 5120
GROUP_COLS = 768


def rope_tables(positions):
    inv_freq = 1.0 / (ROPE_BASE ** (jnp.arange(0, HEAD_DIM, 2, dtype=jnp.float32) / HEAD_DIM))
    angles = positions.astype(jnp.float32)[:, None] * inv_freq[None, :]
    cos, sin = jnp.cos(angles), jnp.sin(angles)
    return jnp.concatenate([cos, cos], axis=-1), jnp.concatenate([-sin, sin], axis=-1)


def rope(x, cos, sin):
    return (x * cos + pltpu.roll(x, HEAD_DIM // 2, 1) * sin).astype(jnp.bfloat16)


def clipped(acc):
    return jnp.clip(acc.astype(jnp.bfloat16), -CLIP_VALUE, CLIP_VALUE)


def kv_kernel(h_ref, scale_ref, w0_ref, w1_ref, cos_ref, sin_ref, normed_ref, kv_ref):
    x = h_ref[...].astype(jnp.float32)
    centred = x - jnp.mean(x, axis=-1, keepdims=True)
    variance = jnp.mean(centred * centred, axis=-1, keepdims=True)
    normed = (centred * lax.rsqrt(variance + NORM_EPS) * scale_ref[...]).astype(jnp.bfloat16)
    normed_ref[...] = normed
    for g, w_ref in enumerate((w0_ref, w1_ref)):
        y = clipped(jnp.dot(normed, w_ref[...], preferred_element_type=jnp.float32))
        kv_ref[:, g * 256:g * 256 + 128] = rope(y[:, :128].astype(jnp.float32), cos_ref[...], sin_ref[...])
        kv_ref[:, g * 256 + 128:g * 256 + 256] = y[:, 128:]


def q_kernel(n_ref, w0_ref, w1_ref, w2_ref, w3_ref, cos_ref, sin_ref, q_ref):
    for i, w_ref in enumerate((w0_ref, w1_ref, w2_ref, w3_ref)):
        y = clipped(jnp.dot(n_ref[...], w_ref[...], preferred_element_type=jnp.float32)).astype(jnp.float32)
        for h in range(2):
            q_ref[:, i * 256 + h * 128:i * 256 + h * 128 + 128] = rope(y[:, h * 128:h * 128 + 128], cos_ref[...], sin_ref[...])


N_TILE = 512
N_TILES = DIM // N_TILE
MESH = pl.DeviceIdType.MESH


def fused_kernel(q_ref, kv_ref, a1_ref, b0_ref, b1_ref, r1_ref, r2_ref, w_ref, hid_ref,
                 out_ref, wg_ref,
                 kvs, o_own, o_in, acc, wbuf, hbuf, att, m_ref, l_ref,
                 z_send, z_recv, p_send, p_recv, o_send, o_recv, kv_sem, w_sem, h_sem):
    dp, tp, cp = lax.axis_index("dp"), lax.axis_index("tp"), lax.axis_index("cp")
    y, core = cp // 2, cp % 2
    to_x, to_y, to_core = {"dp": 1 - dp}, {"cp": (1 - y) * 2 + core}, {"cp": y * 2 + 1 - core}
    to_z, from_z = {"tp": (tp + 1) % 4}, {"tp": (tp + 3) % 4}

    def piece(fx, fy, fc):
        return (1 - dp if fx else dp) * 4 + (1 - y if fy else y) * 2 + (1 - core if fc else core)

    def part(k, idx, off=0, n=128):
        return wg_ref.at[k - 1, pl.ds(pl.multiple_of(idx * 128 + off, 64), n)]

    mine, at_x, at_y, at_xy = piece(0, 0, 0), piece(1, 0, 0), piece(0, 1, 0), piece(1, 1, 0)
    own = {1: r1_ref, 2: r2_ref, 3: part(3, mine)}

    def plane(k, slot):
        src, dst, dev = {
            0: lambda: (own[k], part(k, mine), to_x),
            1: lambda: (own[k], part(k, mine), to_y),
            2: lambda: (own[k], part(k, mine), to_core),
            3: lambda: (part(k, at_x, 0, 64), part(k, at_x, 0, 64), to_y),
            4: lambda: (part(k, at_y, 64, 64), part(k, at_y, 64, 64), to_x),
            5: lambda: (part(k, at_x), part(k, at_x), to_core),
            6: lambda: (part(k, at_y), part(k, at_y), to_core),
            7: lambda: (part(k, at_xy), part(k, at_xy), to_core),
        }[slot]()
        return pltpu.make_async_remote_copy(src_ref=src, dst_ref=dst, send_sem=p_send.at[k - 1, slot], recv_sem=p_recv.at[k - 1, slot], device_id=dev, device_id_type=MESH)

    def arrived(k, slot):
        dst = {
            0: lambda: part(k, at_x), 1: lambda: part(k, at_y), 2: lambda: part(k, piece(0, 0, 1)),
            3: lambda: part(k, at_xy, 0, 64), 4: lambda: part(k, at_xy, 64, 64),
            5: lambda: part(k, piece(1, 0, 1)), 6: lambda: part(k, piece(0, 1, 1)), 7: lambda: part(k, piece(1, 1, 1)),
        }[slot]()
        pltpu.make_async_remote_copy(src_ref=dst, dst_ref=dst, send_sem=p_send.at[k - 1, slot], recv_sem=p_recv.at[k - 1, slot], device_id=to_core, device_id_type=MESH).wait_recv()

    def send_own(k):
        for slot in (0, 1, 2):
            plane(k, slot).start()

    def forward(k):
        arrived(k, 0)
        arrived(k, 1)
        for slot in (3, 4, 5, 6):
            plane(k, slot).start()

    def forward_diag(k):
        arrived(k, 3)
        arrived(k, 4)
        plane(k, 7).start()

    def wait_core(k):
        for slot in (2, 5, 6, 7):
            arrived(k, slot)

    z_copy = pltpu.make_async_remote_copy(src_ref=r2_ref, dst_ref=part(3, mine), send_sem=z_send, recv_sem=z_recv, device_id=to_z, device_id_type=MESH)

    def chunk_rows(c):
        return pl.ds(pl.multiple_of(c * CHUNK, CHUNK), CHUNK)

    def hop(h, c):
        rows = chunk_rows(c)
        src = o_own.at[rows] if h == 1 else o_in.at[h - 2, rows]
        return pltpu.make_async_remote_copy(src_ref=src, dst_ref=o_in.at[h - 1, rows], send_sem=o_send.at[h - 1, c], recv_sem=o_recv.at[h - 1, c], device_id=to_z, device_id_type=MESH)

    def pass_on(h, c):
        hop(h, c).wait_recv()
        if h < 3:
            hop(h + 1, c).start()

    def load_own_weights():
        def body(j, _):
            cols = pl.ds(pl.multiple_of(j * N_TILE, N_TILE), N_TILE)
            pltpu.make_async_copy(w_ref.at[:, cols], wbuf.at[j], w_sem.at[j]).start()
            return 0
        lax.fori_loop(0, N_TILES, body, 0)

    def load_weights(k):
        def body(j, _):
            cols = pl.ds(pl.multiple_of(j * N_TILE, N_TILE), N_TILE)
            for flip in range(8):
                idx = piece(flip // 4, flip // 2 % 2, flip % 2)
                rows = pl.ds(pl.multiple_of(idx * 128, 128), 128)
                src = own[k].at[:, cols] if flip == 0 else wg_ref.at[k - 1, rows, cols]
                pltpu.make_async_copy(src, wbuf.at[j, rows], w_sem.at[j]).start()
            return 0
        lax.fori_loop(0, N_TILES, body, 0)

    def h_copy(c):
        return pltpu.make_async_copy(hid_ref.at[pl.ds(c * CHUNK, CHUNK)], hbuf.at[c % 2], h_sem.at[0, c % 2])

    def out_copy(c):
        return pltpu.make_async_copy(hbuf.at[c % 2], out_ref.at[pl.ds(c * CHUNK, CHUNK)], h_sem.at[1, c % 2])

    barrier = pltpu.get_barrier_semaphore()
    for dev in (to_x, to_y, to_core, to_z, from_z):
        pl.semaphore_signal(barrier, inc=1, device_id=dev, device_id_type=MESH)
    pl.semaphore_wait(barrier, 5)

    z_copy.start()
    send_own(1)
    for i, ref in enumerate((kv_ref, a1_ref, b0_ref, b1_ref)):
        pltpu.make_async_copy(ref, kvs.at[pl.ds(i * ROWS, ROWS)], kv_sem).start()
    send_own(2)
    load_own_weights()
    h_copy(0).start()
    h_copy(1).start()
    pltpu.make_async_copy(kvs, kvs, kv_sem).wait()

    remote_base = jnp.where(cp == 2, 2 * ROWS, ROWS)
    remote_tiles = 2 * cp

    def attend(c, g):
        q_rows = chunk_rows(c)
        lanes = lambda off: pl.ds(pl.multiple_of(g * 512 + off, 128), 128)
        kv_lanes = lambda off: pl.ds(pl.multiple_of(g * 256 + off, 128), 128)
        q = jnp.concatenate([q_ref[q_rows, lanes(h * 128)] for h in range(4)], axis=0)

        def scores(start):
            k = kvs[pl.ds(start, 512), kv_lanes(0)]
            return lax.dot_general(q, k, (((1,), (1,)), ((), ())), preferred_element_type=jnp.float32) * SCALE2

        def weighted(p, start):
            return jnp.dot(p.astype(jnp.bfloat16), kvs[pl.ds(start, 512), kv_lanes(128)], preferred_element_type=jnp.float32)

        def lane_sum(p):
            return (p[:, :128] + p[:, 128:256]) + (p[:, 256:384] + p[:, 384:])

        local = c // 2
        start = pl.multiple_of(local * 512, 512)
        s = scores(start)
        row = lax.broadcasted_iota(jnp.int32, s.shape, 0) % CHUNK + (c % 2) * CHUNK
        col = lax.broadcasted_iota(jnp.int32, s.shape, 1)
        s = jnp.where(col <= row, s, MASK_VALUE)
        m = jnp.broadcast_to(jnp.max(s, axis=-1, keepdims=True), (4 * CHUNK, 128))
        p = jnp.exp2(s - jnp.concatenate([m] * 4, axis=1))
        m_ref[...] = m
        l_ref[...] = lane_sum(p)
        att[...] = weighted(p, start)

        def tile(t, _):
            start = pl.multiple_of(jnp.where(t < local, t * 512, remote_base + (t - local) * 512), 512)
            s = scores(start)
            m_old = m_ref[...]
            m_new = jnp.maximum(m_old, jnp.max(s, axis=-1, keepdims=True))
            rescale = jnp.exp2(m_old - m_new)
            p = jnp.exp2(s - jnp.concatenate([m_new] * 4, axis=1))
            m_ref[...] = m_new
            l_ref[...] = l_ref[...] * rescale + lane_sum(p)
            att[...] = att[...] * rescale + weighted(p, start)
            return 0

        lax.fori_loop(0, local + remote_tiles, tile, 0)
        o = (att[...] / jnp.sum(l_ref[...], axis=-1, keepdims=True)).astype(jnp.bfloat16)
        for h in range(4):
            o_own[q_rows, lanes(h * 128)] = o[h * CHUNK:(h + 1) * CHUNK]

    def chunk(c, _):
        def group(g, _):
            attend(c, g)
            return 0
        lax.fori_loop(0, 2, group, 0)
        hop(1, c).start()

        @pl.when(c == 1)
        def _():
            forward(1)
            z_copy.wait_recv()
            send_own(3)

        @pl.when(c == 2)
        def _():
            pass_on(1, 0)

        @pl.when(c == 3)
        def _():
            pass_on(1, 1)
            forward(2)
        return 0

    lax.fori_loop(0, N_CHUNKS, chunk, 0)

    def stage(k, lo, hi):
        def body(j, _):
            pltpu.make_async_copy(wbuf.at[j], wbuf.at[j], w_sem.at[j]).wait()
            d = jnp.dot(o_own[...] if k == 0 else o_in[k - 1], wbuf[j], preferred_element_type=jnp.float32)
            acc[j] = d if k == 0 else acc[j] + d
            return 0
        lax.fori_loop(lo, hi, body, 0)

    stage(0, 0, 5)
    pass_on(1, 2)
    forward_diag(1)
    stage(0, 5, 10)
    wait_core(1)
    load_weights(1)
    pass_on(1, 3)
    pass_on(2, 0)
    stage(1, 0, 5)
    pass_on(2, 1)
    forward(3)
    stage(1, 5, 10)
    forward_diag(2)
    wait_core(2)
    load_weights(2)
    pass_on(2, 2)
    pass_on(2, 3)
    stage(2, 0, 5)
    forward_diag(3)
    stage(2, 5, 10)
    wait_core(3)
    load_weights(3)

    for c in range(N_CHUNKS):
        rows = pl.ds(c * CHUNK, CHUNK)
        h_copy(c).wait()
        pass_on(3, c)

        def last(j, _, c=c, rows=rows):
            if c == 0:
                pltpu.make_async_copy(wbuf.at[j], wbuf.at[j], w_sem.at[j]).wait()
            cols = pl.ds(pl.multiple_of(j * N_TILE, N_TILE), N_TILE)
            d = acc[j, rows] + jnp.dot(o_in[2, rows], wbuf[j], preferred_element_type=jnp.float32)
            hbuf[c % 2, :, cols] = (hbuf[c % 2, :, cols].astype(jnp.float32) + d).astype(jnp.bfloat16)
            return 0
        lax.fori_loop(0, N_TILES, last, 0)
        out_copy(c).start()
        if c + 2 < N_CHUNKS:
            out_copy(c).wait()
            h_copy(c + 2).start()

    out_copy(2).wait()
    out_copy(3).wait()
    z_copy.wait_send()
    for k in (1, 2, 3):
        for slot in range(8):
            plane(k, slot).wait_send()
        for c in range(N_CHUNKS):
            hop(k, c).wait_send()


def cost(flops, nbytes):
    return pl.CostEstimate(flops=flops, bytes_accessed=nbytes, transcendentals=0)


def once(shape, index_map):
    return pl.BlockSpec(shape, index_map, pipeline_mode=pl.Buffered(1))


def project_kv(hidden, norm_scale, w_qkv, cos, sin):
    tm = 128
    row = lambda i: (i, 0)
    return pl.pallas_call(
        kv_kernel,
        grid=(ROWS // tm,),
        in_specs=[pl.BlockSpec((tm, DIM), row), once((1, DIM), lambda i: (0, 0)), once((DIM, 256), lambda i: (0, 2)), once((DIM, 256), lambda i: (0, 5)), pl.BlockSpec((tm, 128), row), pl.BlockSpec((tm, 128), row)],
        out_specs=[pl.BlockSpec((tm, DIM), row), pl.BlockSpec((tm, 512), row)],
        out_shape=[jax.ShapeDtypeStruct((ROWS, DIM), jnp.bfloat16), jax.ShapeDtypeStruct((ROWS, 512), jnp.bfloat16)],
        compiler_params=pltpu.CompilerParams(vmem_limit_bytes=48 * 2 ** 20),
        cost_estimate=cost(2 * ROWS * DIM * 512, 26 * 2 ** 20),
        name="kv_proj",
    )(hidden, norm_scale.reshape(1, DIM), w_qkv, w_qkv, cos, sin)


def project_q(normed, w_qkv, cos, sin):
    tm = 256
    row = lambda i: (i, 0)
    return pl.pallas_call(
        q_kernel,
        grid=(ROWS // tm,),
        in_specs=[pl.BlockSpec((tm, DIM), row)] + [once((DIM, 256), functools.partial(lambda b, i: (0, b), b)) for b in (0, 1, 3, 4)] + [pl.BlockSpec((tm, 128), row)] * 2,
        out_specs=pl.BlockSpec((tm, 1024), row),
        out_shape=jax.ShapeDtypeStruct((ROWS, 1024), jnp.bfloat16),
        compiler_params=pltpu.CompilerParams(vmem_limit_bytes=48 * 2 ** 20),
        cost_estimate=cost(2 * ROWS * DIM * 1024, 22 * 2 ** 20),
        name="q_proj",
    )(normed, w_qkv, w_qkv, w_qkv, w_qkv, cos, sin)


def fused(q, kv, a1, b0, b1, r1, r2, w_out, hidden):
    hbm = pl.BlockSpec(memory_space=pltpu.HBM)
    vmem = pl.BlockSpec(memory_space=pltpu.VMEM)
    dma = pltpu.SemaphoreType.DMA
    return pl.pallas_call(
        fused_kernel,
        in_specs=[vmem] + [hbm] * 8,
        out_specs=[hbm, hbm],
        out_shape=[jax.ShapeDtypeStruct((ROWS, DIM), jnp.bfloat16), jax.ShapeDtypeStruct((3, ROWS, DIM), jnp.bfloat16)],
        scratch_shapes=[
            pltpu.VMEM((4 * ROWS, 512), jnp.bfloat16),
            pltpu.VMEM((ROWS, ROWS), jnp.bfloat16),
            pltpu.VMEM((3, ROWS, ROWS), jnp.bfloat16),
            pltpu.VMEM((N_TILES, ROWS, N_TILE), jnp.float32),
            pltpu.VMEM((N_TILES, ROWS, N_TILE), jnp.bfloat16),
            pltpu.VMEM((2, CHUNK, DIM), jnp.bfloat16),
            pltpu.VMEM((4 * CHUNK, 128), jnp.float32),
            pltpu.VMEM((4 * CHUNK, 128), jnp.float32),
            pltpu.VMEM((4 * CHUNK, 128), jnp.float32),
            dma, dma, dma((3, 8)), dma((3, 8)), dma((3, 4)), dma((3, 4)), dma, dma((N_TILES,)), dma((2, 2)),
        ],
        compiler_params=pltpu.CompilerParams(collective_id=0, has_side_effects=True, vmem_limit_bytes=63 * 2 ** 20),
        cost_estimate=cost(60 * 10 ** 9, 80 * 2 ** 20),
        name="attend_project",
    )(q, kv, a1, b0, b1, r1, r2, w_out, hidden)[0]


def solution(mesh):
    tok_spec = P(("dp", "cp"), None)
    cache_spec = P(("dp", "cp"), "tp", None)
    ring = [(i, (i + 1) % 4) for i in range(4)]
    shift_z = functools.partial(lax.ppermute, axis_name="tp", perm=ring)

    def local_fn(hidden, norm_scale, w_qkv, w_out):
        cp = lax.axis_index("cp")
        p = lax.axis_index("dp") * 4 + cp
        cos, sin = rope_tables(cp * ROWS + jnp.arange(ROWS))

        w_slice = lax.dynamic_slice(w_out, (p * 128, 0), (128, DIM))
        r1 = shift_z(w_slice)
        normed, kv = project_kv(hidden, norm_scale, w_qkv, cos, sin)
        a1 = lax.ppermute(kv, "cp", [(0, 1), (2, 3)])
        b0 = lax.ppermute(kv, "cp", [(0, 2), (1, 3)])
        q = project_q(normed, w_qkv, cos, sin)
        r1, q = lax.optimization_barrier((r1, q))
        r2 = shift_z(r1)
        b0, q = lax.optimization_barrier((b0, q))
        b1 = lax.ppermute(b0, "cp", [(2, 3), (3, 2)])
        h_out = fused(q, kv, a1, b0, b1, r1, r2, w_out, hidden)

        kv4 = kv.reshape(ROWS, 2, 2, HEAD_DIM)
        return h_out, kv4[:, :, 0], kv4[:, :, 1]

    return jax.shard_map(local_fn, mesh=mesh, in_specs=(tok_spec, P(None), P(None, "tp"), P("tp", None)), out_specs=(tok_spec, cache_spec, cache_spec), check_vma=False)
```
